32 devices in a mesh: gx: 4 (over z), gy: 4 (over x, core), gz: 2 (over y).
Axes of the slice: x: 2, y: 2, z: 4, core: 2. Of those that a mesh axis runs over, the one named last changes fastest.
Arguments:
- hidden_in: bfloat16 [2048, 4096], P(('gx', 'gy'), 'gz'), may hold values from -40 to 40
- norm_gain: float32 [4096], P('gz'), may hold values from 0.25 to 1.75
- normed_grad: bfloat16 [2048, 4096], P(('gx', 'gy'), 'gz'), may hold values from -64 to 64
- key_grad: bfloat16 [2048, 512], P(('gx', 'gy')), may hold values from -6 to 6
- weight_blocks: bfloat16 [16, 2, 520, 128], P(('gx', 'gy'), 'gz'), may hold values from -0.09375 to 0.09375
- block_count: int32 [2, 16], P('gz'), may hold values from 1 to 520, as said below
Outputs:
- hidden_grad: bfloat16 [2048, 4096], P(('gx', 'gy'), 'gz')
- weight_grad: float32 [16, 2, 520, 128], P(('gx', 'gy'), 'gz')
The draws below stay inside these ranges and needn't reach their ends.
Inputs may be any that keep to these rules, and one draw needn't show every extreme that they name: `block_count`: each row sums to 8192; in each row the owners i * 4 to i * 4 + 3 hold together exactly the blocks i * 2048 to min((i + 1) * 2048, 8192) - 1, and one of them holds exactly 520 blocks.
All inputs are finite; a program needn't handle non-finite values.
Results may differ from the reference program's by a relative error of at most 0.0029.
Values may be sent and summed in bfloat16 or wider, within the bound.
A program may use at most 64 MiB of HBM per device.

```python
import math
import jax
import jax.numpy as jnp
from jax import lax

D = 4096
KVW = 512
TOK_DEV = 128
OUTER = 4
INNER = 4
OWNERS = 16
TOKENS = 2048
QUARTERS = 2
BLOCKS = 8192
GROUPB = 2048
MAXB = 520


def joint_activations(key):
    subkeys = jax.random.split(jax.random.fold_in(key, 7001), 5)
    position = jnp.arange(D, dtype=jnp.float32) / D
    base = jnp.clip(jax.random.normal(subkeys[0], (TOKENS, D), jnp.float32), -4.0, 4.0)
    column = jnp.power(3.0, position) * jnp.exp(jax.random.uniform(subkeys[1], (D,), jnp.float32, math.log(0.6), math.log(1.6)))
    hidden = base * column[None, :]
    coefficient = jax.random.uniform(subkeys[3], (TOKENS, 1), jnp.float32, -1.5, 1.5)
    noise = 0.5 * jnp.clip(jax.random.normal(subkeys[4], (TOKENS, D), jnp.float32), -4.0, 4.0)
    return (hidden, coefficient * hidden + noise)


def draw_hidden_in(key, part):
    hidden, _ = joint_activations(key)
    return hidden.astype(jnp.bfloat16)


def draw_normed_grad(key, part):
    _, cotangent = joint_activations(key)
    return cotangent.astype(jnp.bfloat16)


def draw_block_count(key, part):
    subkeys = jax.random.split(jax.random.fold_in(key, 7002), 2)
    group_ids = jnp.arange(OUTER, dtype=jnp.int32)
    totals = jnp.minimum(GROUPB, BLOCKS - group_ids * GROUPB).astype(jnp.int32)
    totals = jnp.broadcast_to(totals[None, :, None], (QUARTERS, OUTER, 1))
    chosen = jax.random.randint(subkeys[0], (QUARTERS, OUTER, 1), 0, INNER, dtype=jnp.int32)
    member = jnp.arange(INNER, dtype=jnp.int32)[None, None, :]
    is_full = member == chosen
    raw_weight = jax.random.randint(subkeys[1], (QUARTERS, OUTER, INNER), 1, 6, dtype=jnp.int32)
    weights = jnp.where(is_full, 0, raw_weight * raw_weight * raw_weight)
    extra = totals - MAXB - (INNER - 1)
    share = extra * weights // jnp.sum(weights, axis=2, keepdims=True)
    share = jnp.minimum(share, MAXB - 1)
    leftover = extra - jnp.sum(share, axis=2, keepdims=True)
    room = jnp.where(is_full, 0, MAXB - 1 - share)
    before = jnp.cumsum(room, axis=2) - room
    share = share + jnp.clip(leftover - before, 0, room)
    counts = jnp.where(is_full, MAXB, 1 + share)
    return counts.reshape(QUARTERS, OWNERS).astype(jnp.int32)


def block_levels(stream_key, dims, cuts, low, largest):
    factor_of = 1.0
    for dim, blocks in cuts:
        steps = jax.random.uniform(jax.random.fold_in(jax.random.fold_in(stream_key, 6), dim), (blocks,), jnp.float32, low / len(cuts), largest / len(cuts))
        factor_of = factor_of * jnp.repeat(jnp.exp(steps), dims[dim] // blocks).reshape((-1,) + (1,) * (len(dims) - 1 - dim))
    return factor_of


def scatter_about(rng, dims, deviation, most, cuts=(), held_as=jnp.bfloat16):
    loudness = block_levels(rng, dims, cuts, -0.22, 0.18) if cuts else 1.0
    result = jax.random.normal(rng, dims, jnp.float32) * deviation * loudness
    return jnp.minimum(jnp.maximum(result, -most), most).astype(held_as)


def setup_inputs(seed: int = 0) -> dict:
    seeds = jax.random.split(jax.random.key(seed), 7)
    return {
        "hidden_in": draw_hidden_in(jax.random.fold_in(seeds[6], 71), 0),
        "norm_gain": jnp.clip(1.0 + 0.15 * jax.random.normal(seeds[1], (D,), jnp.float32), 0.25, 1.75),
        "normed_grad": draw_normed_grad(jax.random.fold_in(seeds[6], 71), 0),
        "key_grad": scatter_about(seeds[3], (TOKENS, KVW), 1.0, 6.0, ((0, 16),)),
        "weight_blocks": scatter_about(seeds[4], (OWNERS, QUARTERS, MAXB, 128), D ** -0.5, 0.09375, ((0, 16), (1, 2))),
        "block_count": draw_block_count(jax.random.fold_in(seeds[6], 71), 0),
    }


EPS = 1e-06

def block_layout(counts):
    ends = jnp.cumsum(counts).astype(jnp.int32)
    starts = (ends - counts).astype(jnp.int32)
    block_ids = jnp.arange(BLOCKS, dtype=jnp.int32)
    owner = jnp.searchsorted(ends, block_ids, side='right').astype(jnp.int32)
    gather_index = (owner * MAXB + block_ids - starts[owner]).astype(jnp.int32)
    slot_owner = jnp.arange(OWNERS * MAXB, dtype=jnp.int32) // MAXB
    slot_within = jnp.arange(OWNERS * MAXB, dtype=jnp.int32) % MAXB
    valid = slot_within < counts[slot_owner]
    source = jnp.clip(starts[slot_owner] + slot_within, 0, BLOCKS - 1).astype(jnp.int32)
    return (gather_index, source, valid)

def reference(hidden_in, norm_gain, normed_grad, key_grad, weight_blocks, block_count):
    group_rows = D // QUARTERS
    pieces = []
    layouts = []
    for group in range(QUARTERS):
        gather_index, source, valid = block_layout(block_count[group])
        layouts.append((source, valid))
        rows = weight_blocks[:, group].reshape(OWNERS * MAXB, 128)
        pieces.append(rows[gather_index].reshape(group_rows, KVW))
    weight = jnp.concatenate(pieces, axis=0)
    gain = norm_gain.astype(jnp.float32)

    def step(total, items):
        hblock, nblock, kblock = items
        hfloat = hblock.astype(jnp.float32)
        rstd = lax.rsqrt(lax.optimization_barrier(jnp.sum(hfloat * hfloat, axis=1)) / D + EPS)
        normed = (hfloat * rstd[:, None] * gain).astype(jnp.bfloat16)
        total = total + lax.dot_general(normed, kblock, (((0,), (0,)), ((), ())), preferred_element_type=jnp.float32)
        dnorm = nblock.astype(jnp.float32) + lax.dot_general(kblock, weight, (((1,), (1,)), ((), ())), preferred_element_type=jnp.float32)
        proj = lax.optimization_barrier(jnp.sum(gain * dnorm * hfloat, axis=1))
        grad = gain * dnorm * rstd[:, None] - hfloat * (rstd ** 3 * proj / D)[:, None]
        return (total, grad.astype(jnp.bfloat16))
    hsplit = hidden_in.reshape(OWNERS, TOK_DEV, D)
    nsplit = normed_grad.reshape(OWNERS, TOK_DEV, D)
    ksplit = key_grad.reshape(OWNERS, TOK_DEV, KVW)
    dweight, grads = lax.scan(step, jnp.zeros((D, KVW), jnp.float32), (hsplit, nsplit, ksplit))
    outs = []
    for group in range(QUARTERS):
        source, valid = layouts[group]
        flat = dweight[group * group_rows:(group + 1) * group_rows].reshape(BLOCKS, 128)
        padded = jnp.where(valid[:, None], flat[source], jnp.float32(0.0))
        outs.append(padded.reshape(OWNERS, MAXB, 128))
    weight_grad = jnp.stack(outs, axis=1)
    return (grads.reshape(TOKENS, D), weight_grad)
```

```python
import functools
import jax
import jax.numpy as jnp
from jax import lax
from jax.experimental import pallas as pl
from jax.experimental.pallas import tpu as pltpu
from jax.sharding import PartitionSpec as P

EPS = 1e-06
LANE = 128
MESH = pl.DeviceIdType.MESH
VMEM_BUDGET = 48 * 2**20


def owner_windows(outer, inner, blocks, most, per_row, rows):
    group = -(-blocks // outer)
    lows, highs = [], []
    for i in range(outer):
        total = min(group, blocks - i * group)
        for j in range(inner):
            low = max(j, total - (inner - j) * most)
            high = min(min(j * most, total - (inner - j)) + most, total)
            lows.append((i * group + low) // per_row // 8 * 8)
            highs.append(-(-(i * group + high) // per_row))
    height = -(-max(h - l for l, h in zip(lows, highs)) // 16) * 16
    return [min(low, rows - height) for low in lows], height


def fast_kernel(
    dims, windows,
    count_ref, hidden_ref, gain_ref, ngrad_ref, key_ref, wb_ref,
    hgrad_ref, wgrad_ref,
    kall, nt_send, nt_recv, pt_send, pt_recv, feat, wpad, wflat, wwin, dacc, dflat,
    sq_send, sq_recv, pj_send, pj_recv,
    own_sem, z_send, z_recv, s1_send, s1_recv, s2_send, s2_recv, s3_send, s3_recv,
    n_send, n_recv, p_send, p_recv, e_send, e_recv,
):
    outer, inner, model_width, most, per_row, height, pad = dims
    f32, bf16 = jnp.float32, jnp.bfloat16
    a, b, g = lax.axis_index("gx"), lax.axis_index("gy"), lax.axis_index("gz")
    x, c = b // 2, b % 2
    ox, oc, og = 1 - x, 1 - c, 1 - g
    me = a * inner + b
    tokens, rows = hidden_ref.shape
    owners = outer * inner
    chunks = rows // LANE
    half = tokens // 2

    def peer(rel, k):
        px = ox if k // 2 else x
        pc = oc if k % 2 else c
        return lax.rem(a + rel, outer), px, pc

    def remote(src, dst, send, recv, gx, gy, gz):
        return pltpu.make_async_remote_copy(
            src_ref=src, dst_ref=dst, send_sem=send, recv_sem=recv,
            device_id=(gx, gy, gz), device_id_type=MESH)

    pairs = [(rel, k) for rel in range(outer) for k in range(inner) if rel or k]
    barrier = pltpu.get_barrier_semaphore()
    for rel, k in pairs:
        pa, px, pc = peer(rel, k)
        pl.semaphore_signal(barrier, inc=1, device_id=(pa, px * 2 + pc, g), device_id_type=MESH)
    pl.semaphore_signal(barrier, inc=1, device_id=(a, b, og), device_id_type=MESH)

    own = [pltpu.make_async_copy(key_ref.at[pl.ds(h * half, half)], kall.at[a, c, h, x], own_sem.at[h])
           for h in range(2)]
    for copy in own:
        copy.start()

    squares = jnp.zeros((tokens, LANE), f32)
    for i in range(chunks):
        part = hidden_ref[:, i * LANE:(i + 1) * LANE].astype(f32)
        squares = squares + part * part
    row_sum = jnp.sum(squares, axis=1, keepdims=True)
    sq_send[...] = jnp.broadcast_to(row_sum, (tokens, LANE)).T[0:8, :]
    for copy in own:
        copy.wait()
    pl.semaphore_wait(barrier, owners)

    sends = []

    def start(copy):
        copy.start()
        sends.append(copy)
        return copy

    sq_copy = start(remote(sq_send, sq_recv, e_send.at[0], e_recv.at[0], a, b, og))
    zc = {}
    for rel in range(1, outer):
        piece = kall.at[a, c, g, x]
        zc[rel] = start(remote(piece, piece, z_send.at[rel], z_recv.at[rel],
                               lax.rem(a - rel + outer, outer), b, g))
    bx, bc = ox * 2 + c, x * 2 + oc
    own_piece = kall.at[a, c, g, x]
    step1 = {0: start(remote(own_piece, own_piece, s1_send.at[0], s1_recv.at[0], a, bx, g))}
    step2, step3 = {}, {}

    begin = jnp.int32(0)
    window_low = jnp.int32(0)
    count = jnp.int32(0)
    for o in range(owners):
        value = count_ref[0, o]
        begin = begin + jnp.where(o < me, value, 0)
        count = count + jnp.where(me == o, value, 0)
        window_low = window_low + jnp.where(me == o, windows[o], 0)
    offset = jnp.clip(begin - window_low * per_row, 0, pad)
    flat_rows = height * per_row
    slot = lax.broadcasted_iota(jnp.int32, (most, LANE), 0)
    wpad[...] = jnp.zeros_like(wpad)
    wpad[pad:pad + most, :] = jnp.where(slot < count, wb_ref[...].astype(f32), 0.0)
    wflat[...] = wpad[pl.ds(pad - offset, flat_rows), :]
    for i in range(per_row):
        wwin[:, i * LANE:(i + 1) * LANE] = wflat[pl.ds(i, height, stride=per_row), :].astype(bf16)

    sq_copy.wait_recv()
    total = row_sum + jnp.broadcast_to(sq_recv[0:1, :], (tokens, LANE)).T[:, 0:1]
    rstd = lax.rsqrt(total / model_width + EPS)

    for rel in range(1, outer):
        zc[rel].wait_recv()
        s = lax.rem(a + rel, outer)
        piece = kall.at[s, c, g, x]
        to = (a, bx, g) if rel % 2 else (a, b, og)
        step1[rel] = start(remote(piece, piece, s1_send.at[rel], s1_recv.at[rel], *to))

    for i in range(chunks):
        cols = slice(i * LANE, (i + 1) * LANE)
        normed = hidden_ref[:, cols].astype(f32) * rstd * gain_ref[:, cols]
        feat[cols, :] = normed.T
    for o in range(owners):
        nt_send[o] = feat[windows[o]:windows[o] + height, :].astype(bf16)
    nc = {}
    for rel, k in pairs:
        pa, px, pc = peer(rel, k)
        nc[rel, k] = start(remote(
            nt_send.at[pa * inner + px * 2 + pc], nt_recv.at[me],
            n_send.at[rel * inner + k], n_recv.at[rel * inner + k], pa, px * 2 + pc, g))

    for rel in range(outer):
        step1[rel].wait_recv()
        s = lax.rem(a + rel, outer)
        if rel == 0:
            piece, to = kall.at[s, c, g, ox], (a, b, og)
        elif rel % 2:
            piece, to = kall.at[s, c, g], (a, b, og)
        else:
            piece, to = kall.at[s, c, :, x], (a, bx, g)
        step2[rel] = start(remote(piece, piece, s2_send.at[rel], s2_recv.at[rel], *to))
    for rel in range(outer):
        step2[rel].wait_recv()
        piece = kall.at[lax.rem(a + rel, outer), c]
        step3[rel] = start(remote(piece, piece, s3_send.at[rel], s3_recv.at[rel], a, bc, g))

    def keys(s, px, pc):
        return jnp.concatenate([kall[s, pc, 0, px], kall[s, pc, 1, px]], axis=0)

    pc_copies = {}
    for rel in range(outer):
        step3[rel].wait_recv()
        for k in range(inner):
            pa, px, pc = peer(rel, k)
            to = pa * inner + px * 2 + pc
            product = lax.dot_general(
                wwin[...], keys(pa, px, pc), (((1,), (1,)), ((), ())),
                preferred_element_type=f32).astype(bf16)
            if rel == 0 and k == 0:
                pt_recv[me] = product
            else:
                pt_send[to] = product
                pc_copies[rel, k] = start(remote(
                    pt_send.at[to], pt_recv.at[me],
                    p_send.at[rel * inner + k], p_recv.at[rel * inner + k], pa, px * 2 + pc, g))

    for rel in range(outer):
        for k in range(inner):
            pa, px, pc = peer(outer - rel, k)
            source = pa * inner + px * 2 + pc
            if rel == 0 and k == 0:
                part = nt_send[source]
            else:
                nc[rel, k].wait_recv()
                part = nt_recv[source]
            term = jnp.dot(part, keys(pa, px, pc), preferred_element_type=f32)
            if rel == 0 and k == 0:
                dacc[...] = term
            else:
                dacc[...] += term
    for i in range(per_row):
        dflat[pl.ds(i, height, stride=per_row), :] = dacc[:, i * LANE:(i + 1) * LANE]
    dflat[flat_rows:, :] = jnp.zeros((most, LANE), f32)
    wgrad_ref[...] = jnp.where(slot < count, dflat[pl.ds(offset, most), :], 0.0)

    for rel, k in pairs:
        pc_copies[rel, k].wait_recv()
    feat[...] = jnp.zeros_like(feat)
    for o in range(owners):
        feat[windows[o]:windows[o] + height, :] += pt_recv[o].astype(f32)
    proj = jnp.zeros((tokens, LANE), f32)
    for i in range(chunks):
        cols = slice(i * LANE, (i + 1) * LANE)
        gained = gain_ref[:, cols] * (ngrad_ref[:, cols].astype(f32) + feat[cols, :].T)
        feat[cols, :] = gained
        proj = proj + gained * hidden_ref[:, cols].astype(f32)
    proj_sum = jnp.sum(proj, axis=1, keepdims=True)
    pj_send[...] = jnp.broadcast_to(proj_sum, (tokens, LANE)).T[0:8, :]
    pj_copy = start(remote(pj_send, pj_recv, e_send.at[1], e_recv.at[1], a, b, og))
    pj_copy.wait_recv()
    proj_all = proj_sum + jnp.broadcast_to(pj_recv[0:1, :], (tokens, LANE)).T[:, 0:1]
    scale = rstd * rstd * rstd * proj_all / model_width
    for i in range(chunks):
        cols = slice(i * LANE, (i + 1) * LANE)
        grad = feat[cols, :] * rstd - hidden_ref[:, cols].astype(f32) * scale
        hgrad_ref[:, cols] = grad.astype(bf16)
    for copy in sends:
        copy.wait_send()


def fast_plan(mesh, hidden, key, wb):
    outer, inner, halves = (mesh.shape[n] for n in ("gx", "gy", "gz"))
    tokens, rows, width, most = hidden.shape[0], hidden.shape[1], key.shape[1], wb.shape[2]
    if inner != 4 or halves != 2 or tokens != LANE or rows % LANE or width % LANE or most % 8:
        return None
    per_row = width // LANE
    windows, height = owner_windows(outer, inner, rows * per_row, most, per_row, rows)
    if rows % 16 or min(windows) < 0:
        return None
    held = outer * inner * (tokens * width * 2 + 4 * height * tokens * 2) + 6 * tokens * rows * 4
    if held > VMEM_BUDGET:
        return None
    return windows, height, per_row


def fast_shards(mesh, plan, hidden_in, norm_gain, normed_grad, key_grad, weight_blocks, block_count):
    windows, height, per_row = plan
    outer, inner = mesh.shape["gx"], mesh.shape["gy"]
    owners = outer * inner
    tokens, rows = hidden_in.shape
    width, most = key_grad.shape[1], weight_blocks.shape[2]
    model_width = rows * mesh.shape["gz"]
    flat_rows = height * per_row
    group = -(-rows * per_row // outer)
    pad = -(-max(
        i * group + min(j * most, group) - windows[i * inner + j] * per_row
        for i in range(outer) for j in range(inner)) // 8) * 8
    dims = (outer, inner, model_width, most, per_row, height, pad)
    f32, bf16 = jnp.float32, jnp.bfloat16
    vmem, dma = pltpu.VMEM, pltpu.SemaphoreType.DMA
    in_vmem = pl.BlockSpec(memory_space=pltpu.VMEM)
    hgrad, wgrad = pl.pallas_call(
        functools.partial(fast_kernel, dims, windows),
        out_shape=(jax.ShapeDtypeStruct((tokens, rows), bf16), jax.ShapeDtypeStruct((most, LANE), f32)),
        in_specs=[pl.BlockSpec(memory_space=pltpu.SMEM)] + [in_vmem] * 5,
        out_specs=(in_vmem, in_vmem),
        scratch_shapes=[
            vmem((outer, 2, 2, 2, tokens // 2, width), bf16),
            vmem((owners, height, tokens), bf16), vmem((owners, height, tokens), bf16),
            vmem((owners, height, tokens), bf16), vmem((owners, height, tokens), bf16),
            vmem((rows, tokens), f32),
            vmem((pad + max(flat_rows, most), LANE), f32), vmem((flat_rows, LANE), f32),
            vmem((height, width), bf16), vmem((height, width), f32), vmem((flat_rows + most, LANE), f32),
            vmem((8, LANE), f32), vmem((8, LANE), f32), vmem((8, LANE), f32), vmem((8, LANE), f32),
            dma((2,)),
        ] + [dma((outer,))] * 8 + [dma((owners,))] * 4 + [dma((2,))] * 2,
        compiler_params=pltpu.CompilerParams(
            collective_id=0, has_side_effects=True, vmem_limit_bytes=VMEM_BUDGET),
    )(block_count, hidden_in, norm_gain.reshape(1, rows), normed_grad, key_grad,
      weight_blocks.reshape(most, LANE))
    return hgrad, wgrad.reshape(1, 1, most, LANE)


def block_layout(counts, blocks, owners, most):
    ends = jnp.cumsum(counts)
    starts = ends - counts
    block_ids = jnp.arange(blocks, dtype=jnp.int32)
    owner = jnp.searchsorted(ends, block_ids, side="right")
    gather_index = owner * most + block_ids - starts[owner]
    slot_owner = jnp.arange(owners * most, dtype=jnp.int32) // most
    slot_within = jnp.arange(owners * most, dtype=jnp.int32) % most
    valid = slot_within < counts[slot_owner]
    source = jnp.clip(starts[slot_owner] + slot_within, 0, blocks - 1)
    return (gather_index, source, valid)


def select_rows(index, keep, rows):
    columns = jnp.arange(rows.shape[0], dtype=jnp.int32)
    onehot = (index[:, None] == columns[None, :]) & keep[:, None]
    if rows.dtype == jnp.bfloat16:
        picked = jnp.dot(onehot.astype(jnp.bfloat16), rows, preferred_element_type=jnp.float32)
        return picked.astype(jnp.bfloat16)
    return jnp.dot(
        onehot.astype(jnp.float32),
        rows,
        precision=lax.Precision.HIGHEST,
        preferred_element_type=jnp.float32,
    )


def select_groups(index, keep, rows):

    def one_group(items):
        return select_rows(items[0], items[1], items[2])

    return lax.map(one_group, (index, keep, rows))


def shards(hidden_in, norm_gain, normed_grad, key_grad, weight_blocks, block_count):
    outer_size = lax.axis_size("gx")
    inner_size = lax.axis_size("gy")
    owners = outer_size * inner_size
    most = weight_blocks.shape[2]
    group_slots_count = inner_size * most
    group_rows = hidden_in.shape[1]
    width = key_grad.shape[1]
    blocks = group_rows * width // 128
    group_blocks = (blocks + outer_size - 1) // outer_size
    model_width = group_rows * lax.axis_size("gz")
    gather_index, source, valid = block_layout(block_count[0], blocks, owners, most)
    outer_index = lax.axis_index("gx")
    padded_index = jnp.pad(gather_index, (0, outer_size * group_blocks - blocks), mode="edge")
    group_offsets = jnp.arange(outer_size, dtype=jnp.int32)[:, None]
    local_index = jnp.clip(
        padded_index.reshape(outer_size, group_blocks) - group_offsets * group_slots_count,
        0,
        group_slots_count - 1,
    )
    local_source = jnp.clip(
        source.reshape(outer_size, group_slots_count) - group_offsets * group_blocks,
        0,
        group_blocks - 1,
    )
    local_valid = valid.reshape(outer_size, group_slots_count)
    all_rows = jnp.ones((outer_size, group_blocks), dtype=bool)
    local_blocks = weight_blocks.reshape(most, 128)
    gathered = lax.all_gather(local_blocks, ("gx", "gy"), axis=0, tiled=True)
    dense = select_groups(
        local_index, all_rows, gathered.reshape(outer_size, group_slots_count, 128)
    )
    weight = dense.reshape(outer_size * group_blocks, 128)[:blocks].reshape(group_rows, width)
    hfloat = hidden_in.astype(jnp.float32)
    squares = lax.psum(jnp.sum(hfloat * hfloat, axis=1), "gz")
    rstd = lax.rsqrt(squares / model_width + EPS)
    normed = (hfloat * rstd[:, None] * norm_gain).astype(jnp.bfloat16)
    dnorm = normed_grad.astype(jnp.float32) + lax.dot_general(
        key_grad, weight, (((1,), (1,)), ((), ())), preferred_element_type=jnp.float32
    )
    proj = lax.psum(jnp.sum(norm_gain * dnorm * hfloat, axis=1), "gz")
    grad = norm_gain * dnorm * rstd[:, None] - hfloat * (rstd**3 * proj / model_width)[:, None]
    hidden_grad = grad.astype(jnp.bfloat16)
    dweight = lax.dot_general(
        normed, key_grad, (((0,), (0,)), ((), ())), preferred_element_type=jnp.float32
    )
    flat = dweight.reshape(blocks, 128)
    flat_padded = jnp.pad(flat, ((0, outer_size * group_blocks - blocks), (0, 0)))
    group_sum = lax.psum_scatter(flat_padded, "gx", scatter_dimension=0, tiled=True)
    slot_source = lax.dynamic_index_in_dim(local_source, outer_index, 0, keepdims=False)
    slot_valid = lax.dynamic_index_in_dim(local_valid, outer_index, 0, keepdims=False)
    slotted = select_rows(slot_source, slot_valid, group_sum)
    owned = lax.psum_scatter(slotted, "gy", scatter_dimension=0, tiled=True)
    return (hidden_grad, owned.reshape(1, 1, most, 128))


def solution(mesh):
    placed = (
        P(("gx", "gy"), "gz"),
        P("gz"),
        P(("gx", "gy"), "gz"),
        P(("gx", "gy"), None),
        P(("gx", "gy"), "gz", None, None),
        P("gz", None),
    )

    def body(*args):
        plan = fast_plan(mesh, args[0], args[3], args[4])
        if plan is None:
            return shards(*args)
        return fast_shards(mesh, plan, *args)

    return jax.shard_map(
        body,
        mesh=mesh,
        in_specs=placed,
        out_specs=(P(("gx", "gy"), "gz"), P(("gx", "gy"), "gz", None, None)),
        check_vma=False,
    )
```

```python
import functools
import jax
import jax.numpy as jnp
from jax import lax
from jax.experimental import pallas as pl
from jax.experimental.pallas import tpu as pltpu
from jax.sharding import PartitionSpec as P

EPS = 1e-06
LANE = 128
MESH = pl.DeviceIdType.MESH
VMEM_BUDGET = 48 * 2**20


def owner_windows(inner, group, most, per_row):
    lows, highs = [], []
    for j in range(inner):
        low = max(j, group - (inner - j) * most)
        high = min(min(j * most, group - (inner - j)) + most, group)
        lows.append(low // per_row // 8 * 8)
        highs.append(-(-high // per_row))
    height = -(-max(h - l for l, h in zip(lows, highs)) // 16) * 16
    return [min(low, group // per_row - height) for low in lows], height


def fast_kernel(
    dims, windows,
    count_ref, gain_ref, hidden_hbm, ngrad_hbm, key_hbm, wb_hbm,
    hgrad_ref, wgrad_ref,
    hidden_ref, ngrad_ref, wb_ref, kplane, kz, nt_send, nt_recv, pt_send, pt_recv, feat, wpad, wflat,
    wz, dacc, dwin, drecv1, dsum, drecv2, dflat, sq_send, sq_recv, pj_send, pj_recv,
    in_sem, w_send, w_recv, k_send, k_recv, y_send, y_recv, x_send, x_recv,
    n_send, n_recv, p_send, p_recv, d_send, d_recv, e_send, e_recv,
):
    outer, inner, model_width, most, per_row, height, pad = dims
    f32, bf16 = jnp.float32, jnp.bfloat16
    a, b, g = lax.axis_index("gx"), lax.axis_index("gy"), lax.axis_index("gz")
    x, c = b // 2, b % 2
    ox, oc, og = 1 - x, 1 - c, 1 - g
    me = a * inner + b
    bx, bc = ox * 2 + c, x * 2 + oc
    tokens, rows = hidden_ref.shape
    owners = outer * inner
    chunks = rows // LANE
    half = tokens // 2
    group_rows = rows // outer
    flat_rows = height * per_row

    def remote(src, dst, send, recv, gx, gy, gz):
        return pltpu.make_async_remote_copy(
            src_ref=src, dst_ref=dst, send_sem=send, recv_sem=recv,
            device_id=(gx, gy, gz), device_id_type=MESH)

    loads = [
        pltpu.make_async_copy(wb_hbm, wb_ref, in_sem.at[0]),
        pltpu.make_async_copy(hidden_hbm, hidden_ref, in_sem.at[1]),
        pltpu.make_async_copy(key_hbm, kplane.at[c, x], in_sem.at[2]),
        pltpu.make_async_copy(key_hbm.at[pl.ds(0, half)], kz.at[a, 0], in_sem.at[3]),
        pltpu.make_async_copy(key_hbm.at[pl.ds(half, half)], kz.at[a, 1], in_sem.at[4]),
        pltpu.make_async_copy(ngrad_hbm, ngrad_ref, in_sem.at[5]),
    ]
    for load in loads:
        load.start()

    def gy_peer(k):
        return (ox if k // 2 else x), (oc if k % 2 else c)

    barrier = pltpu.get_barrier_semaphore()
    for rel in range(1, outer):
        pl.semaphore_signal(barrier, inc=1, device_id=(lax.rem(a + rel, outer), b, g), device_id_type=MESH)
    for k in range(1, inner):
        px, pc = gy_peer(k)
        pl.semaphore_signal(barrier, inc=1, device_id=(a, px * 2 + pc, g), device_id_type=MESH)
    pl.semaphore_signal(barrier, inc=1, device_id=(a, b, og), device_id_type=MESH)

    begin = jnp.int32(0)
    count = jnp.int32(0)
    for o in range(owners):
        value = count_ref[0, o]
        begin = begin + jnp.where(o < me, value, 0)
        count = count + jnp.where(me == o, value, 0)
    window_low = a * group_rows
    for j in range(inner):
        window_low = window_low + jnp.where(b == j, windows[j], 0)
    offset = jnp.clip(begin - window_low * per_row, 0, pad)
    slot = lax.broadcasted_iota(jnp.int32, (most, LANE), 0)
    wpad[...] = jnp.zeros_like(wpad)
    loads[0].wait()
    wpad[pad:pad + most, :] = jnp.where(slot < count, wb_ref[...].astype(f32), 0.0)
    wflat[...] = wpad[pl.ds(pad - offset, flat_rows), :]
    for i in range(per_row):
        wz[a, :, i * LANE:(i + 1) * LANE] = wflat[pl.ds(i, height, stride=per_row), :].astype(bf16)

    loads[1].wait()
    squares = jnp.zeros((tokens, LANE), f32)
    for i in range(chunks):
        part = hidden_ref[:, i * LANE:(i + 1) * LANE].astype(f32)
        squares = squares + part * part
    row_sum = jnp.sum(squares, axis=1, keepdims=True)
    sq_send[...] = jnp.broadcast_to(row_sum, (tokens, LANE)).T[0:8, :]
    for load in loads[2:5]:
        load.wait()
    pl.semaphore_wait(barrier, outer + inner - 1)

    sends = []

    def start(make, when=None):
        sends.append((make, when))
        if when is None:
            make().start()
        else:
            pl.when(when)(lambda: make().start())

    def right(piece, send, recv, t):
        def make():
            return remote(piece(a - t), piece(a - t), send.at[t], recv.at[t], a + 1, b, g)
        start(make, (a - t >= 0) & (a + 1 < outer))

    def left(piece, send, recv, t):
        at = outer - 1 + t
        def make():
            return remote(piece(a + t), piece(a + t), send.at[at], recv.at[at], a - 1, b, g)
        start(make, (a + t < outer) & (a >= 1))

    def arrived(piece, send, recv, t, after=None):
        at = outer - 1 + t
        def from_left():
            s = a - 1 - t
            remote(piece(s), piece(s), send.at[t], recv.at[t], a - 1, b, g).wait_recv()
            if after is not None:
                after(s)
        def from_right():
            s = a + 1 + t
            remote(piece(s), piece(s), send.at[at], recv.at[at], a + 1, b, g).wait_recv()
            if after is not None:
                after(s)
        pl.when(a - 1 - t >= 0)(from_left)
        pl.when(a + 1 + t < outer)(from_right)

    def w_piece(s):
        return wz.at[s]

    def k_piece(s):
        return kz.at[s, g]

    def sq_copy():
        return remote(sq_send, sq_recv, e_send.at[0], e_recv.at[0], a, b, og)

    def kx_copy():
        return remote(kplane.at[c, x], kplane.at[c, x], x_send.at[0], x_recv.at[0], a, bx, g)

    def kc_copy():
        return remote(kplane.at[c], kplane.at[c], x_send.at[1], x_recv.at[1], a, bc, g)

    def y_copy(s):
        return remote(kz.at[s, g], kz.at[s, g], y_send.at[s], y_recv.at[s], a, b, og)

    start(sq_copy)
    start(kx_copy)
    for piece, send, recv in ((w_piece, w_send, w_recv), (k_piece, k_send, k_recv)):
        right(piece, send, recv, 0)
        left(piece, send, recv, 0)

    sq_copy().wait_recv()
    total = row_sum + jnp.broadcast_to(sq_recv[0:1, :], (tokens, LANE)).T[:, 0:1]
    rstd = lax.rsqrt(total / model_width + EPS)
    for i in range(chunks):
        cols = slice(i * LANE, (i + 1) * LANE)
        normed = hidden_ref[:, cols].astype(f32) * rstd * gain_ref[:, cols]
        first = i * LANE
        nt_send[first // group_rows, first % group_rows:first % group_rows + LANE, :] = normed.T.astype(bf16)

    def n_copy(rel):
        to = lax.rem(a + rel, outer)
        return lambda: remote(nt_send.at[to], nt_recv.at[a], n_send.at[rel], n_recv.at[rel], to, b, g)

    for rel in range(1, outer):
        start(n_copy(rel))

    def relay(t):
        arrived(w_piece, w_send, w_recv, t)
        if t + 1 < outer - 1:
            right(w_piece, w_send, w_recv, t + 1)
            left(w_piece, w_send, w_recv, t + 1)
        arrived(k_piece, k_send, k_recv, t, lambda s: y_copy(s).start())
        if t + 1 < outer - 1:
            right(k_piece, k_send, k_recv, t + 1)
            left(k_piece, k_send, k_recv, t + 1)

    def p_copy(s, k):
        px, pc = gy_peer(k)
        return remote(pt_send.at[s, k], pt_recv.at[s, b], p_send.at[s * inner + k],
                      p_recv.at[s * inner + k], a, px * 2 + pc, g)

    def products(s):
        for k in (2, 3, 1, 0):
            px, pc = gy_peer(k)
            product = lax.dot_general(
                wz[s], kplane[pc, px], (((1,), (1,)), ((), ())), preferred_element_type=f32)
            if k == 0:
                pt_recv[s, b] = product
            else:
                pt_send[s, k] = product
                p_copy(s, k).start()

    relay(0)
    kx_copy().wait_recv()
    start(kc_copy)
    kc_copy().wait_recv()
    products(a)
    for t in range(outer - 1):
        if t:
            relay(t)
        pl.when(a - 1 - t >= 0)(functools.partial(products, a - 1 - t))
        pl.when(a + 1 + t < outer)(functools.partial(products, a + 1 + t))

    nt_recv[a] = nt_send[a]
    for rel in range(1, outer):
        y_copy(lax.rem(a + rel, outer)).wait_recv()
        n_copy(rel)().wait_recv()
    dacc[...] = jnp.dot(
        jnp.concatenate([nt_recv[s] for s in range(outer)], axis=1),
        kz[...].reshape(outer * tokens, kz.shape[-1]), preferred_element_type=f32)
    for j in range(inner):
        dwin[j % 2, j // 2] = dacc[windows[j]:windows[j] + height, :]

    def dc_copy():
        return remote(dwin.at[oc], drecv1, d_send.at[0], d_recv.at[0], a, bc, g)

    def dx_copy():
        return remote(dsum.at[ox], drecv2, d_send.at[1], d_recv.at[1], a, bx, g)

    start(dc_copy)
    dc_copy().wait_recv()
    dsum[ox] = dwin[c, ox] + drecv1[ox]
    start(dx_copy)
    dsum[x] = dwin[c, x] + drecv1[x]

    for rel in range(outer):
        for k in range(1, inner):
            p_copy(lax.rem(a + rel, outer), k).wait_recv()
    loads[5].wait()
    feat[...] = jnp.zeros_like(feat)
    for s in range(outer):
        for j in range(inner):
            low = s * group_rows + windows[j]
            feat[low:low + height, :] += pt_recv[s, j]
    proj = jnp.zeros((tokens, LANE), f32)
    for i in range(chunks):
        cols = slice(i * LANE, (i + 1) * LANE)
        gained = gain_ref[:, cols] * (ngrad_ref[:, cols].astype(f32) + feat[cols, :].T)
        feat[cols, :] = gained
        proj = proj + gained * hidden_ref[:, cols].astype(f32)
    proj_sum = jnp.sum(proj, axis=1, keepdims=True)
    pj_send[...] = jnp.broadcast_to(proj_sum, (tokens, LANE)).T[0:8, :]

    def pj_copy():
        return remote(pj_send, pj_recv, e_send.at[1], e_recv.at[1], a, b, og)

    start(pj_copy)

    dx_copy().wait_recv()
    for i in range(per_row):
        cols = slice(i * LANE, (i + 1) * LANE)
        dflat[pl.ds(i, height, stride=per_row), :] = dsum[x, :, cols] + drecv2[:, cols]
    dflat[flat_rows:, :] = jnp.zeros((most, LANE), f32)
    wgrad_ref[...] = jnp.where(slot < count, dflat[pl.ds(offset, most), :], 0.0)

    pj_copy().wait_recv()
    proj_all = proj_sum + jnp.broadcast_to(pj_recv[0:1, :], (tokens, LANE)).T[:, 0:1]
    scale = rstd * rstd * rstd * proj_all / model_width
    for i in range(chunks):
        cols = slice(i * LANE, (i + 1) * LANE)
        grad = feat[cols, :] * rstd - hidden_ref[:, cols].astype(f32) * scale
        hgrad_ref[:, cols] = grad.astype(bf16)
    for make, when in sends:
        if when is None:
            make().wait_send()
        else:
            pl.when(when)(lambda make=make: make().wait_send())
    for rel in range(outer):
        s = lax.rem(a + rel, outer)
        if rel:
            y_copy(s).wait_send()
        for k in range(1, inner):
            p_copy(s, k).wait_send()


def fast_plan(mesh, hidden, key, wb):
    outer, inner, halves = (mesh.shape[n] for n in ("gx", "gy", "gz"))
    tokens, rows, width, most = hidden.shape[0], hidden.shape[1], key.shape[1], wb.shape[2]
    if inner != 4 or halves != 2 or tokens != LANE or width % LANE or most % 8:
        return None
    per_row = width // LANE
    if rows % (outer * LANE):
        return None
    group = rows // outer * per_row
    windows, height = owner_windows(inner, group, most, per_row)
    if min(windows) < 0:
        return None
    held = outer * (
        4 * tokens * width + rows // outer * (4 * tokens + 4 * width) + inner * height * tokens * 8
        + height * width * 2) + 6 * height * width * 4 * 2 + tokens * rows * 12
    if held > VMEM_BUDGET:
        return None
    return windows, height, per_row, group


def fast_shards(mesh, plan, hidden_in, norm_gain, normed_grad, key_grad, weight_blocks, block_count):
    windows, height, per_row, group = plan
    outer, inner = mesh.shape["gx"], mesh.shape["gy"]
    tokens, rows = hidden_in.shape
    width, most = key_grad.shape[1], weight_blocks.shape[2]
    model_width = rows * mesh.shape["gz"]
    flat_rows = height * per_row
    pad = -(-max(min(j * most, group - inner + j) - windows[j] * per_row for j in range(inner)) // 8) * 8
    dims = (outer, inner, model_width, most, per_row, height, pad)
    f32, bf16 = jnp.float32, jnp.bfloat16
    vmem, dma = pltpu.VMEM, pltpu.SemaphoreType.DMA
    in_vmem = pl.BlockSpec(memory_space=pltpu.VMEM)
    in_hbm = pl.BlockSpec(memory_space=pltpu.HBM)
    hgrad, wgrad = pl.pallas_call(
        functools.partial(fast_kernel, dims, windows),
        out_shape=(jax.ShapeDtypeStruct((tokens, rows), bf16), jax.ShapeDtypeStruct((most, LANE), f32)),
        in_specs=[pl.BlockSpec(memory_space=pltpu.SMEM), in_vmem] + [in_hbm] * 4,
        out_specs=(in_vmem, in_vmem),
        scratch_shapes=[
            vmem((tokens, rows), bf16), vmem((tokens, rows), bf16), vmem((most, LANE), bf16),
            vmem((2, 2, tokens, width), bf16), vmem((outer, 2, tokens // 2, width), bf16),
            vmem((outer, rows // outer, tokens), bf16), vmem((outer, rows // outer, tokens), bf16),
            vmem((outer, inner, height, tokens), f32), vmem((outer, inner, height, tokens), f32),
            vmem((rows, tokens), f32),
            vmem((pad + max(flat_rows, most), LANE), f32), vmem((flat_rows, LANE), f32),
            vmem((outer, height, width), bf16), vmem((rows // outer, width), f32),
            vmem((2, 2, height, width), f32), vmem((2, height, width), f32), vmem((2, height, width), f32),
            vmem((height, width), f32), vmem((flat_rows + most, LANE), f32),
            vmem((8, LANE), f32), vmem((8, LANE), f32), vmem((8, LANE), f32), vmem((8, LANE), f32),
            dma((6,)),
        ] + [dma((2 * (outer - 1),))] * 4 + [dma((outer,))] * 2 + [dma((2,))] * 2
        + [dma((outer,))] * 2 + [dma((outer * inner,))] * 2 + [dma((2,))] * 4,
        compiler_params=pltpu.CompilerParams(
            collective_id=0, has_side_effects=True, vmem_limit_bytes=VMEM_BUDGET),
    )(block_count, norm_gain.reshape(1, rows), hidden_in, normed_grad, key_grad,
      weight_blocks.reshape(most, LANE))
    return hgrad, wgrad.reshape(1, 1, most, LANE)


def block_layout(counts, blocks, owners, most):
    ends = jnp.cumsum(counts)
    starts = ends - counts
    block_ids = jnp.arange(blocks, dtype=jnp.int32)
    owner = jnp.searchsorted(ends, block_ids, side="right")
    gather_index = owner * most + block_ids - starts[owner]
    slot_owner = jnp.arange(owners * most, dtype=jnp.int32) // most
    slot_within = jnp.arange(owners * most, dtype=jnp.int32) % most
    valid = slot_within < counts[slot_owner]
    source = jnp.clip(starts[slot_owner] + slot_within, 0, blocks - 1)
    return (gather_index, source, valid)


def select_rows(index, keep, rows):
    columns = jnp.arange(rows.shape[0], dtype=jnp.int32)
    onehot = (index[:, None] == columns[None, :]) & keep[:, None]
    if rows.dtype == jnp.bfloat16:
        picked = jnp.dot(onehot.astype(jnp.bfloat16), rows, preferred_element_type=jnp.float32)
        return picked.astype(jnp.bfloat16)
    return jnp.dot(
        onehot.astype(jnp.float32),
        rows,
        precision=lax.Precision.HIGHEST,
        preferred_element_type=jnp.float32,
    )


def select_groups(index, keep, rows):

    def one_group(items):
        return select_rows(items[0], items[1], items[2])

    return lax.map(one_group, (index, keep, rows))


def shards(hidden_in, norm_gain, normed_grad, key_grad, weight_blocks, block_count):
    outer_size = lax.axis_size("gx")
    inner_size = lax.axis_size("gy")
    owners = outer_size * inner_size
    most = weight_blocks.shape[2]
    group_slots_count = inner_size * most
    group_rows = hidden_in.shape[1]
    width = key_grad.shape[1]
    blocks = group_rows * width // 128
    group_blocks = (blocks + outer_size - 1) // outer_size
    model_width = group_rows * lax.axis_size("gz")
    gather_index, source, valid = block_layout(block_count[0], blocks, owners, most)
    outer_index = lax.axis_index("gx")
    padded_index = jnp.pad(gather_index, (0, outer_size * group_blocks - blocks), mode="edge")
    group_offsets = jnp.arange(outer_size, dtype=jnp.int32)[:, None]
    local_index = jnp.clip(
        padded_index.reshape(outer_size, group_blocks) - group_offsets * group_slots_count,
        0,
        group_slots_count - 1,
    )
    local_source = jnp.clip(
        source.reshape(outer_size, group_slots_count) - group_offsets * group_blocks,
        0,
        group_blocks - 1,
    )
    local_valid = valid.reshape(outer_size, group_slots_count)
    all_rows = jnp.ones((outer_size, group_blocks), dtype=bool)
    local_blocks = weight_blocks.reshape(most, 128)
    gathered = lax.all_gather(local_blocks, ("gx", "gy"), axis=0, tiled=True)
    dense = select_groups(
        local_index, all_rows, gathered.reshape(outer_size, group_slots_count, 128)
    )
    weight = dense.reshape(outer_size * group_blocks, 128)[:blocks].reshape(group_rows, width)
    hfloat = hidden_in.astype(jnp.float32)
    squares = lax.psum(jnp.sum(hfloat * hfloat, axis=1), "gz")
    rstd = lax.rsqrt(squares / model_width + EPS)
    normed = (hfloat * rstd[:, None] * norm_gain).astype(jnp.bfloat16)
    dnorm = normed_grad.astype(jnp.float32) + lax.dot_general(
        key_grad, weight, (((1,), (1,)), ((), ())), preferred_element_type=jnp.float32
    )
    proj = lax.psum(jnp.sum(norm_gain * dnorm * hfloat, axis=1), "gz")
    grad = norm_gain * dnorm * rstd[:, None] - hfloat * (rstd**3 * proj / model_width)[:, None]
    hidden_grad = grad.astype(jnp.bfloat16)
    dweight = lax.dot_general(
        normed, key_grad, (((0,), (0,)), ((), ())), preferred_element_type=jnp.float32
    )
    flat = dweight.reshape(blocks, 128)
    flat_padded = jnp.pad(flat, ((0, outer_size * group_blocks - blocks), (0, 0)))
    group_sum = lax.psum_scatter(flat_padded, "gx", scatter_dimension=0, tiled=True)
    slot_source = lax.dynamic_index_in_dim(local_source, outer_index, 0, keepdims=False)
    slot_valid = lax.dynamic_index_in_dim(local_valid, outer_index, 0, keepdims=False)
    slotted = select_rows(slot_source, slot_valid, group_sum)
    owned = lax.psum_scatter(slotted, "gy", scatter_dimension=0, tiled=True)
    return (hidden_grad, owned.reshape(1, 1, most, 128))


def solution(mesh):
    placed = (
        P(("gx", "gy"), "gz"),
        P("gz"),
        P(("gx", "gy"), "gz"),
        P(("gx", "gy"), None),
        P(("gx", "gy"), "gz", None, None),
        P("gz", None),
    )

    def body(*args):
        plan = fast_plan(mesh, args[0], args[3], args[4])
        if plan is None:
            return shards(*args)
        return fast_shards(mesh, plan, *args)

    return jax.shard_map(
        body,
        mesh=mesh,
        in_specs=placed,
        out_specs=(P(("gx", "gy"), "gz"), P(("gx", "gy"), "gz", None, None)),
        check_vma=False,
    )
```

```python
import functools
import jax
import jax.numpy as jnp
from jax import lax
from jax.experimental import pallas as pl
from jax.experimental.pallas import tpu as pltpu
from jax.sharding import PartitionSpec as P

EPS = 1e-06
LANE = 128
MESH = pl.DeviceIdType.MESH
VMEM_BUDGET = 48 * 2**20


def owner_windows(inner, group, most, per_row):
    lows, highs = [], []
    for j in range(inner):
        low = max(j, group - (inner - j) * most)
        high = min(min(j * most, group - (inner - j)) + most, group)
        lows.append(low // per_row // 8 * 8)
        highs.append(-(-high // per_row))
    height = -(-max(h - l for l, h in zip(lows, highs)) // 16) * 16
    return [min(low, group // per_row - height) for low in lows], height


def fast_kernel(
    dims, windows,
    count_ref, gain_ref, hidden_hbm, ngrad_hbm, key_hbm, wb_hbm,
    hgrad_ref, wgrad_ref,
    hidden_ref, ngrad_ref, wb_ref, kplane, kz, nt_send, nt_recv, pt_send, pt_recv, feat, wpad, wflat,
    wz, dacc, dwin, drecv1, dsum, drecv2, dflat, sq_send, sq_recv, pj_send, pj_recv,
    in_sem, w_send, w_recv, k_send, k_recv, y_send, y_recv, x_send, x_recv,
    n_send, n_recv, p_send, p_recv, d_send, d_recv, e_send, e_recv,
):
    outer, inner, model_width, most, per_row, height, pad, parts, part_rows = dims
    f32, bf16 = jnp.float32, jnp.bfloat16
    a, b, g = lax.axis_index("gx"), lax.axis_index("gy"), lax.axis_index("gz")
    x, c = b // 2, b % 2
    ox, oc, og = 1 - x, 1 - c, 1 - g
    me = a * inner + b
    bx, bc = ox * 2 + c, x * 2 + oc
    tokens, rows = hidden_ref.shape
    owners = outer * inner
    chunks = rows // LANE
    half = tokens // 2
    group_rows = rows // outer
    flat_rows = height * per_row

    def remote(src, dst, send, recv, gx, gy, gz):
        return pltpu.make_async_remote_copy(
            src_ref=src, dst_ref=dst, send_sem=send, recv_sem=recv,
            device_id=(gx, gy, gz), device_id_type=MESH)

    loads = [
        pltpu.make_async_copy(wb_hbm, wb_ref, in_sem.at[0]),
        pltpu.make_async_copy(hidden_hbm, hidden_ref, in_sem.at[1]),
        pltpu.make_async_copy(key_hbm, kplane.at[c, x], in_sem.at[2]),
        pltpu.make_async_copy(key_hbm.at[pl.ds(0, half)], kz.at[a, 0], in_sem.at[3]),
        pltpu.make_async_copy(key_hbm.at[pl.ds(half, half)], kz.at[a, 1], in_sem.at[4]),
        pltpu.make_async_copy(ngrad_hbm, ngrad_ref, in_sem.at[5]),
    ]
    for load in loads:
        load.start()

    def gy_peer(k):
        return (ox if k // 2 else x), (oc if k % 2 else c)

    barrier = pltpu.get_barrier_semaphore()
    for rel in range(1, outer):
        pl.semaphore_signal(barrier, inc=1, device_id=(lax.rem(a + rel, outer), b, g), device_id_type=MESH)
    for k in range(1, inner):
        px, pc = gy_peer(k)
        pl.semaphore_signal(barrier, inc=1, device_id=(a, px * 2 + pc, g), device_id_type=MESH)
    pl.semaphore_signal(barrier, inc=1, device_id=(a, b, og), device_id_type=MESH)

    begin = jnp.int32(0)
    count = jnp.int32(0)
    for o in range(owners):
        value = count_ref[0, o]
        begin = begin + jnp.where(o < me, value, 0)
        count = count + jnp.where(me == o, value, 0)
    window_low = a * group_rows
    for j in range(inner):
        window_low = window_low + jnp.where(b == j, windows[j], 0)
    offset = jnp.clip(begin - window_low * per_row, 0, pad)
    slot = lax.broadcasted_iota(jnp.int32, (most, LANE), 0)
    wpad[...] = jnp.zeros_like(wpad)
    loads[0].wait()
    wpad[pad:pad + most, :] = jnp.where(slot < count, wb_ref[...].astype(f32), 0.0)
    wflat[...] = wpad[pl.ds(pad - offset, flat_rows), :]
    for i in range(per_row):
        wz[a, :, i * LANE:(i + 1) * LANE] = wflat[pl.ds(i, height, stride=per_row), :].astype(bf16)

    for load in loads[2:5]:
        load.wait()
    pl.semaphore_wait(barrier, outer + inner - 1)

    sends = []

    def start(make, when=None):
        sends.append((make, when))
        if when is None:
            make().start()
        else:
            pl.when(when)(lambda: make().start())

    def right(piece, send, recv, t):
        def make():
            return remote(piece(a - t), piece(a - t), send.at[t], recv.at[t], a + 1, b, g)
        start(make, (a - t >= 0) & (a + 1 < outer))

    def left(piece, send, recv, t):
        at = outer - 1 + t
        def make():
            return remote(piece(a + t), piece(a + t), send.at[at], recv.at[at], a - 1, b, g)
        start(make, (a + t < outer) & (a >= 1))

    def arrived(piece, send, recv, t):
        at = outer - 1 + t
        def from_left():
            s = a - 1 - t
            remote(piece(s), piece(s), send.at[t], recv.at[t], a - 1, b, g).wait_recv()
        def from_right():
            s = a + 1 + t
            remote(piece(s), piece(s), send.at[at], recv.at[at], a + 1, b, g).wait_recv()
        pl.when(a - 1 - t >= 0)(from_left)
        pl.when(a + 1 + t < outer)(from_right)

    def w_piece(s):
        return wz.at[s]

    def k_copy(rel):
        to = lax.rem(a + rel, outer)
        return lambda: remote(kz.at[a, g], kz.at[a, g], k_send.at[rel], k_recv.at[rel], to, b, g)

    def sq_copy():
        return remote(sq_send, sq_recv, e_send.at[0], e_recv.at[0], a, b, og)

    def kx_copy():
        return remote(kplane.at[c, x], kplane.at[c, x], x_send.at[0], x_recv.at[0], a, bx, g)

    def kc_copy():
        return remote(kplane.at[c], kplane.at[c], x_send.at[1], x_recv.at[1], a, bc, g)

    def y_copy(s):
        return remote(kz.at[s, g], kz.at[s, g], y_send.at[s], y_recv.at[s], a, b, og)

    start(kx_copy)
    right(w_piece, w_send, w_recv, 0)
    left(w_piece, w_send, w_recv, 0)
    for rel in range(1, outer):
        start(k_copy(rel))

    loads[1].wait()
    squares = jnp.zeros((tokens, LANE), f32)
    for i in range(chunks):
        part = hidden_ref[:, i * LANE:(i + 1) * LANE].astype(f32)
        squares = squares + part * part
    row_sum = jnp.sum(squares, axis=1, keepdims=True)
    sq_send[...] = jnp.broadcast_to(row_sum, (tokens, LANE)).T[0:8, :]
    start(sq_copy)
    sq_copy().wait_recv()
    total = row_sum + jnp.broadcast_to(sq_recv[0:1, :], (tokens, LANE)).T[:, 0:1]
    rstd = lax.rsqrt(total / model_width + EPS)
    for i in range(chunks):
        cols = slice(i * LANE, (i + 1) * LANE)
        normed = hidden_ref[:, cols].astype(f32) * rstd * gain_ref[:, cols]
        turned = normed.T.astype(bf16)
        low = i * LANE % group_rows
        for part in range(2):
            begins = max(low, parts[part])
            ends = min(low + LANE, parts[part] + part_rows)
            if begins < ends:
                nt_send[i * LANE // group_rows, part, begins - parts[part]:ends - parts[part], :] = (
                    turned[begins - low:ends - low, :])

    def n_copy(rel, turn):
        to = lax.rem(a + rel, outer)
        part = x if turn else ox
        at = turn * outer + rel
        return lambda: remote(
            nt_send.at[to, part], nt_recv.at[a, part], n_send.at[at], n_recv.at[at], to, b, g)

    for turn in range(2):
        for rel in range(1, outer):
            start(n_copy(rel, turn))

    def relay(t):
        arrived(w_piece, w_send, w_recv, t)
        if t + 1 < outer - 1:
            right(w_piece, w_send, w_recv, t + 1)
            left(w_piece, w_send, w_recv, t + 1)

    def p_copy(s, k):
        px, pc = gy_peer(k)
        return remote(pt_send.at[s, k], pt_recv.at[s, b], p_send.at[s * inner + k],
                      p_recv.at[s * inner + k], a, px * 2 + pc, g)

    def products(s):
        for k in (2, 3, 1, 0):
            px, pc = gy_peer(k)
            product = lax.dot_general(
                wz[s], kplane[pc, px], (((1,), (1,)), ((), ())), preferred_element_type=f32)
            if k == 0:
                pt_recv[s, b] = product
            else:
                pt_send[s, k] = product
                p_copy(s, k).start()

    def dc_copy(turn):
        part = x if turn else ox
        return lambda: remote(
            dwin.at[part, oc], drecv1.at[part], d_send.at[turn], d_recv.at[turn], a, bc, g)

    def dx_copy():
        return remote(dsum, drecv2, d_send.at[2], d_recv.at[2], a, bx, g)

    def window_sums(turn):
        part = x if turn else ox
        for rel in range(1, outer):
            n_copy(rel, turn)().wait_recv()
        nt_recv[a, part] = nt_send[a, part]
        dacc[...] = jnp.dot(
            jnp.concatenate([nt_recv[s, part] for s in range(outer)], axis=1),
            kz[...].reshape(outer * tokens, kz.shape[-1]), preferred_element_type=f32)
        for pc in range(2):
            low = jnp.where(part == 0, windows[pc] - parts[0], windows[2 + pc] - parts[1])
            dwin[part, pc] = dacc[pl.ds(pl.multiple_of(low, 8), height), :]
        start(dc_copy(turn))

    def products_from(t):
        pl.when(a - 1 - t >= 0)(functools.partial(products, a - 1 - t))
        pl.when(a + 1 + t < outer)(functools.partial(products, a + 1 + t))

    for rel in range(1, outer):
        k_copy(rel)().wait_recv()
        s = lax.rem(a - rel + outer, outer)
        start(functools.partial(y_copy, s))
    kx_copy().wait_recv()
    start(kc_copy)
    relay(0)
    kc_copy().wait_recv()
    products(a)
    products_from(0)
    for t in range(1, outer - 2):
        relay(t)
        products_from(t)
    for rel in range(1, outer):
        y_copy(lax.rem(a + rel, outer)).wait_recv()
    window_sums(0)
    dc_copy(0)().wait_recv()
    dsum[...] = dwin[ox, c] + drecv1[ox]
    start(dx_copy)
    relay(outer - 2)
    products_from(outer - 2)
    window_sums(1)

    for rel in range(outer):
        for k in range(1, inner):
            p_copy(lax.rem(a + rel, outer), k).wait_recv()
    loads[5].wait()
    feat[...] = jnp.zeros_like(feat)
    for s in range(outer):
        for j in range(inner):
            low = s * group_rows + windows[j]
            feat[low:low + height, :] += pt_recv[s, j]
    proj = jnp.zeros((tokens, LANE), f32)
    for i in range(chunks):
        cols = slice(i * LANE, (i + 1) * LANE)
        gained = gain_ref[:, cols] * (ngrad_ref[:, cols].astype(f32) + feat[cols, :].T)
        feat[cols, :] = gained
        proj = proj + gained * hidden_ref[:, cols].astype(f32)
    proj_sum = jnp.sum(proj, axis=1, keepdims=True)
    pj_send[...] = jnp.broadcast_to(proj_sum, (tokens, LANE)).T[0:8, :]

    def pj_copy():
        return remote(pj_send, pj_recv, e_send.at[1], e_recv.at[1], a, b, og)

    start(pj_copy)

    dc_copy(1)().wait_recv()
    dx_copy().wait_recv()
    for i in range(per_row):
        cols = slice(i * LANE, (i + 1) * LANE)
        dflat[pl.ds(i, height, stride=per_row), :] = dwin[x, c, :, cols] + drecv1[x, :, cols] + drecv2[:, cols]
    dflat[flat_rows:, :] = jnp.zeros((most, LANE), f32)
    wgrad_ref[...] = jnp.where(slot < count, dflat[pl.ds(offset, most), :], 0.0)

    pj_copy().wait_recv()
    proj_all = proj_sum + jnp.broadcast_to(pj_recv[0:1, :], (tokens, LANE)).T[:, 0:1]
    scale = rstd * rstd * rstd * proj_all / model_width
    for i in range(chunks):
        cols = slice(i * LANE, (i + 1) * LANE)
        grad = feat[cols, :] * rstd - hidden_ref[:, cols].astype(f32) * scale
        hgrad_ref[:, cols] = grad.astype(bf16)
    for make, when in sends:
        if when is None:
            make().wait_send()
        else:
            pl.when(when)(lambda make=make: make().wait_send())
    for rel in range(outer):
        s = lax.rem(a + rel, outer)
        for k in range(1, inner):
            p_copy(s, k).wait_send()


def fast_plan(mesh, hidden, key, wb):
    outer, inner, halves = (mesh.shape[n] for n in ("gx", "gy", "gz"))
    tokens, rows, width, most = hidden.shape[0], hidden.shape[1], key.shape[1], wb.shape[2]
    if inner != 4 or halves != 2 or tokens != LANE or width % LANE or most % 8:
        return None
    per_row = width // LANE
    if rows % (outer * LANE):
        return None
    group = rows // outer * per_row
    windows, height = owner_windows(inner, group, most, per_row)
    if min(windows) < 0 or rows // outer < 2 * height + 16:
        return None
    held = outer * (
        4 * tokens * width + rows // outer * (4 * tokens + 4 * width) + inner * height * tokens * 8
        + height * width * 2) + 6 * height * width * 4 * 2 + tokens * rows * 12
    if held > VMEM_BUDGET:
        return None
    return windows, height, per_row, group


def fast_shards(mesh, plan, hidden_in, norm_gain, normed_grad, key_grad, weight_blocks, block_count):
    windows, height, per_row, group = plan
    outer, inner = mesh.shape["gx"], mesh.shape["gy"]
    tokens, rows = hidden_in.shape
    width, most = key_grad.shape[1], weight_blocks.shape[2]
    model_width = rows * mesh.shape["gz"]
    flat_rows = height * per_row
    pad = -(-max(min(j * most, group - inner + j) - windows[j] * per_row for j in range(inner)) // 8) * 8
    parts = [min(windows[0:2]), min(windows[2:4])]
    part_rows = max(max(windows[0:2]) - parts[0], max(windows[2:4]) - parts[1]) + height
    part_rows = -(-part_rows // 16) * 16
    parts = [min(low, rows // outer - part_rows) for low in parts]
    dims = (outer, inner, model_width, most, per_row, height, pad, parts, part_rows)
    f32, bf16 = jnp.float32, jnp.bfloat16
    vmem, dma = pltpu.VMEM, pltpu.SemaphoreType.DMA
    in_vmem = pl.BlockSpec(memory_space=pltpu.VMEM)
    in_hbm = pl.BlockSpec(memory_space=pltpu.HBM)
    hgrad, wgrad = pl.pallas_call(
        functools.partial(fast_kernel, dims, windows),
        out_shape=(jax.ShapeDtypeStruct((tokens, rows), bf16), jax.ShapeDtypeStruct((most, LANE), f32)),
        in_specs=[pl.BlockSpec(memory_space=pltpu.SMEM), in_vmem] + [in_hbm] * 4,
        out_specs=(in_vmem, in_vmem),
        scratch_shapes=[
            vmem((tokens, rows), bf16), vmem((tokens, rows), bf16), vmem((most, LANE), bf16),
            vmem((2, 2, tokens, width), bf16), vmem((outer, 2, tokens // 2, width), bf16),
            vmem((outer, 2, part_rows, tokens), bf16), vmem((outer, 2, part_rows, tokens), bf16),
            vmem((outer, inner, height, tokens), f32), vmem((outer, inner, height, tokens), f32),
            vmem((rows, tokens), f32),
            vmem((pad + max(flat_rows, most), LANE), f32), vmem((flat_rows, LANE), f32),
            vmem((outer, height, width), bf16), vmem((part_rows, width), f32),
            vmem((2, 2, height, width), f32), vmem((2, height, width), f32), vmem((height, width), f32),
            vmem((height, width), f32), vmem((flat_rows + most, LANE), f32),
            vmem((8, LANE), f32), vmem((8, LANE), f32), vmem((8, LANE), f32), vmem((8, LANE), f32),
            dma((6,)),
        ] + [dma((2 * (outer - 1),))] * 4 + [dma((outer,))] * 2 + [dma((2,))] * 2
        + [dma((2 * outer,))] * 2 + [dma((outer * inner,))] * 2 + [dma((3,))] * 2 + [dma((2,))] * 2,
        compiler_params=pltpu.CompilerParams(
            collective_id=0, has_side_effects=True),
    )(block_count, norm_gain.reshape(1, rows), hidden_in, normed_grad, key_grad,
      weight_blocks.reshape(most, LANE))
    return hgrad, wgrad.reshape(1, 1, most, LANE)


def block_layout(counts, blocks, owners, most):
    ends = jnp.cumsum(counts)
    starts = ends - counts
    block_ids = jnp.arange(blocks, dtype=jnp.int32)
    owner = jnp.searchsorted(ends, block_ids, side="right")
    gather_index = owner * most + block_ids - starts[owner]
    slot_owner = jnp.arange(owners * most, dtype=jnp.int32) // most
    slot_within = jnp.arange(owners * most, dtype=jnp.int32) % most
    valid = slot_within < counts[slot_owner]
    source = jnp.clip(starts[slot_owner] + slot_within, 0, blocks - 1)
    return (gather_index, source, valid)


def select_rows(index, keep, rows):
    columns = jnp.arange(rows.shape[0], dtype=jnp.int32)
    onehot = (index[:, None] == columns[None, :]) & keep[:, None]
    if rows.dtype == jnp.bfloat16:
        picked = jnp.dot(onehot.astype(jnp.bfloat16), rows, preferred_element_type=jnp.float32)
        return picked.astype(jnp.bfloat16)
    return jnp.dot(
        onehot.astype(jnp.float32),
        rows,
        precision=lax.Precision.HIGHEST,
        preferred_element_type=jnp.float32,
    )


def select_groups(index, keep, rows):

    def one_group(items):
        return select_rows(items[0], items[1], items[2])

    return lax.map(one_group, (index, keep, rows))


def shards(hidden_in, norm_gain, normed_grad, key_grad, weight_blocks, block_count):
    outer_size = lax.axis_size("gx")
    inner_size = lax.axis_size("gy")
    owners = outer_size * inner_size
    most = weight_blocks.shape[2]
    group_slots_count = inner_size * most
    group_rows = hidden_in.shape[1]
    width = key_grad.shape[1]
    blocks = group_rows * width // 128
    group_blocks = (blocks + outer_size - 1) // outer_size
    model_width = group_rows * lax.axis_size("gz")
    gather_index, source, valid = block_layout(block_count[0], blocks, owners, most)
    outer_index = lax.axis_index("gx")
    padded_index = jnp.pad(gather_index, (0, outer_size * group_blocks - blocks), mode="edge")
    group_offsets = jnp.arange(outer_size, dtype=jnp.int32)[:, None]
    local_index = jnp.clip(
        padded_index.reshape(outer_size, group_blocks) - group_offsets * group_slots_count,
        0,
        group_slots_count - 1,
    )
    local_source = jnp.clip(
        source.reshape(outer_size, group_slots_count) - group_offsets * group_blocks,
        0,
        group_blocks - 1,
    )
    local_valid = valid.reshape(outer_size, group_slots_count)
    all_rows = jnp.ones((outer_size, group_blocks), dtype=bool)
    local_blocks = weight_blocks.reshape(most, 128)
    gathered = lax.all_gather(local_blocks, ("gx", "gy"), axis=0, tiled=True)
    dense = select_groups(
        local_index, all_rows, gathered.reshape(outer_size, group_slots_count, 128)
    )
    weight = dense.reshape(outer_size * group_blocks, 128)[:blocks].reshape(group_rows, width)
    hfloat = hidden_in.astype(jnp.float32)
    squares = lax.psum(jnp.sum(hfloat * hfloat, axis=1), "gz")
    rstd = lax.rsqrt(squares / model_width + EPS)
    normed = (hfloat * rstd[:, None] * norm_gain).astype(jnp.bfloat16)
    dnorm = normed_grad.astype(jnp.float32) + lax.dot_general(
        key_grad, weight, (((1,), (1,)), ((), ())), preferred_element_type=jnp.float32
    )
    proj = lax.psum(jnp.sum(norm_gain * dnorm * hfloat, axis=1), "gz")
    grad = norm_gain * dnorm * rstd[:, None] - hfloat * (rstd**3 * proj / model_width)[:, None]
    hidden_grad = grad.astype(jnp.bfloat16)
    dweight = lax.dot_general(
        normed, key_grad, (((0,), (0,)), ((), ())), preferred_element_type=jnp.float32
    )
    flat = dweight.reshape(blocks, 128)
    flat_padded = jnp.pad(flat, ((0, outer_size * group_blocks - blocks), (0, 0)))
    group_sum = lax.psum_scatter(flat_padded, "gx", scatter_dimension=0, tiled=True)
    slot_source = lax.dynamic_index_in_dim(local_source, outer_index, 0, keepdims=False)
    slot_valid = lax.dynamic_index_in_dim(local_valid, outer_index, 0, keepdims=False)
    slotted = select_rows(slot_source, slot_valid, group_sum)
    owned = lax.psum_scatter(slotted, "gy", scatter_dimension=0, tiled=True)
    return (hidden_grad, owned.reshape(1, 1, most, 128))


def solution(mesh):
    placed = (
        P(("gx", "gy"), "gz"),
        P("gz"),
        P(("gx", "gy"), "gz"),
        P(("gx", "gy"), None),
        P(("gx", "gy"), "gz", None, None),
        P("gz", None),
    )

    def body(*args):
        plan = fast_plan(mesh, args[0], args[3], args[4])
        if plan is None:
            return shards(*args)
        return fast_shards(mesh, plan, *args)

    return jax.shard_map(
        body,
        mesh=mesh,
        in_specs=placed,
        out_specs=(P(("gx", "gy"), "gz"), P(("gx", "gy"), "gz", None, None)),
        check_vma=False,
    )
```

```python
import functools
import jax
import jax.numpy as jnp
from jax import lax
from jax.experimental import pallas as pl
from jax.experimental.pallas import tpu as pltpu
from jax.sharding import PartitionSpec as P

EPS = 1e-06
LANE = 128
MESH = pl.DeviceIdType.MESH
VMEM_BUDGET = 48 * 2**20


def owner_windows(outer, inner, blocks, most, per_row, rows):
    group = -(-blocks // outer)
    lows, highs = [], []
    for i in range(outer):
        total = min(group, blocks - i * group)
        for j in range(inner):
            low = max(j, total - (inner - j) * most)
            high = min(min(j * most, total - (inner - j)) + most, total)
            lows.append((i * group + low) // per_row // 8 * 8)
            highs.append(-(-(i * group + high) // per_row))
    height = -(-max(h - l for l, h in zip(lows, highs)) // 16) * 16
    return [min(low, rows - height) for low in lows], height


def fast_kernel(
    dims, windows,
    count_ref, hidden_hbm, gain_ref, ngrad_hbm, key_hbm, wb_hbm,
    hgrad_ref, wgrad_ref,
    hidden_ref, ngrad_ref, wb_ref, kall, nt_send, nt_recv, pt_send, pt_recv, feat, wpad, wflat, wwin, dacc, dflat,
    sq_send, sq_recv, pj_send, pj_recv,
    own_sem, z_send, z_recv, s1_send, s1_recv, s2_send, s2_recv, s3_send, s3_recv,
    n_send, n_recv, p_send, p_recv, e_send, e_recv,
):
    outer, inner, model_width, most, per_row, height, pad = dims
    f32, bf16 = jnp.float32, jnp.bfloat16
    a, b, g = lax.axis_index("gx"), lax.axis_index("gy"), lax.axis_index("gz")
    x, c = b // 2, b % 2
    ox, oc, og = 1 - x, 1 - c, 1 - g
    me = a * inner + b
    tokens, rows = hidden_ref.shape
    owners = outer * inner
    chunks = rows // LANE
    half = tokens // 2

    def peer(rel, k):
        px = ox if k // 2 else x
        pc = oc if k % 2 else c
        return lax.rem(a + rel, outer), px, pc

    def remote(src, dst, send, recv, gx, gy, gz):
        return pltpu.make_async_remote_copy(
            src_ref=src, dst_ref=dst, send_sem=send, recv_sem=recv,
            device_id=(gx, gy, gz), device_id_type=MESH)

    own = [pltpu.make_async_copy(key_hbm.at[pl.ds(h * half, half)], kall.at[a, c, h, x], own_sem.at[h])
           for h in range(2)]
    own += [
        pltpu.make_async_copy(hidden_hbm, hidden_ref, own_sem.at[2]),
        pltpu.make_async_copy(wb_hbm, wb_ref, own_sem.at[3]),
        pltpu.make_async_copy(ngrad_hbm, ngrad_ref, own_sem.at[4]),
    ]
    for copy in own:
        copy.start()

    pairs = [(rel, k) for rel in range(outer) for k in range(inner) if rel or k]
    barrier = pltpu.get_barrier_semaphore()
    for rel, k in pairs:
        pa, px, pc = peer(rel, k)
        pl.semaphore_signal(barrier, inc=1, device_id=(pa, px * 2 + pc, g), device_id_type=MESH)
    pl.semaphore_signal(barrier, inc=1, device_id=(a, b, og), device_id_type=MESH)

    for copy in own[0:2]:
        copy.wait()
    pl.semaphore_wait(barrier, owners)

    sends = []

    def start(copy):
        copy.start()
        sends.append(copy)
        return copy

    zc = {}
    for rel in range(1, outer):
        piece = kall.at[a, c, g, x]
        zc[rel] = start(remote(piece, piece, z_send.at[rel], z_recv.at[rel],
                               lax.rem(a - rel + outer, outer), b, g))
    bx, bc = ox * 2 + c, x * 2 + oc
    own_piece = kall.at[a, c, g, x]
    step1 = {0: start(remote(own_piece, own_piece, s1_send.at[0], s1_recv.at[0], a, bx, g))}
    step2, step3 = {}, {}
    own[2].wait()
    squares = jnp.zeros((tokens, LANE), f32)
    for i in range(chunks):
        part = hidden_ref[:, i * LANE:(i + 1) * LANE].astype(f32)
        squares = squares + part * part
    row_sum = jnp.sum(squares, axis=1, keepdims=True)
    sq_send[...] = jnp.broadcast_to(row_sum, (tokens, LANE)).T[0:8, :]
    sq_copy = start(remote(sq_send, sq_recv, e_send.at[0], e_recv.at[0], a, b, og))

    begin = jnp.int32(0)
    window_low = jnp.int32(0)
    count = jnp.int32(0)
    for o in range(owners):
        value = count_ref[0, o]
        begin = begin + jnp.where(o < me, value, 0)
        count = count + jnp.where(me == o, value, 0)
        window_low = window_low + jnp.where(me == o, windows[o], 0)
    offset = jnp.clip(begin - window_low * per_row, 0, pad)
    flat_rows = height * per_row
    slot = lax.broadcasted_iota(jnp.int32, (most, LANE), 0)
    wpad[...] = jnp.zeros_like(wpad)
    own[3].wait()
    wpad[pad:pad + most, :] = jnp.where(slot < count, wb_ref[...].astype(f32), 0.0)
    wflat[...] = wpad[pl.ds(pad - offset, flat_rows), :]
    for i in range(per_row):
        wwin[:, i * LANE:(i + 1) * LANE] = wflat[pl.ds(i, height, stride=per_row), :].astype(bf16)

    sq_copy.wait_recv()
    total = row_sum + jnp.broadcast_to(sq_recv[0:1, :], (tokens, LANE)).T[:, 0:1]
    rstd = lax.rsqrt(total / model_width + EPS)

    for rel in range(1, outer):
        zc[rel].wait_recv()
        s = lax.rem(a + rel, outer)
        piece = kall.at[s, c, g, x]
        to = (a, bx, g) if rel % 2 else (a, b, og)
        step1[rel] = start(remote(piece, piece, s1_send.at[rel], s1_recv.at[rel], *to))

    for i in range(chunks):
        cols = slice(i * LANE, (i + 1) * LANE)
        normed = hidden_ref[:, cols].astype(f32) * rstd * gain_ref[:, cols]
        feat[cols, :] = normed.T
    for o in range(owners):
        nt_send[o] = feat[windows[o]:windows[o] + height, :].astype(bf16)
    nc = {}
    for rel, k in pairs:
        pa, px, pc = peer(rel, k)
        nc[rel, k] = start(remote(
            nt_send.at[pa * inner + px * 2 + pc], nt_recv.at[me],
            n_send.at[rel * inner + k], n_recv.at[rel * inner + k], pa, px * 2 + pc, g))

    for rel in range(outer):
        step1[rel].wait_recv()
        s = lax.rem(a + rel, outer)
        if rel == 0:
            piece, to = kall.at[s, c, g, ox], (a, b, og)
        elif rel % 2:
            piece, to = kall.at[s, c, g], (a, b, og)
        else:
            piece, to = kall.at[s, c, :, x], (a, bx, g)
        step2[rel] = start(remote(piece, piece, s2_send.at[rel], s2_recv.at[rel], *to))
    for rel in range(outer):
        step2[rel].wait_recv()
        piece = kall.at[lax.rem(a + rel, outer), c]
        step3[rel] = start(remote(piece, piece, s3_send.at[rel], s3_recv.at[rel], a, bc, g))

    def keys(s, px, pc):
        return jnp.concatenate([kall[s, pc, 0, px], kall[s, pc, 1, px]], axis=0)

    pc_copies = {}
    for rel in range(outer):
        step3[rel].wait_recv()
        for k in range(inner):
            pa, px, pc = peer(rel, k)
            to = pa * inner + px * 2 + pc
            product = lax.dot_general(
                wwin[...], keys(pa, px, pc), (((1,), (1,)), ((), ())),
                preferred_element_type=f32).astype(bf16)
            if rel == 0 and k == 0:
                pt_recv[me] = product
            else:
                pt_send[to] = product
                pc_copies[rel, k] = start(remote(
                    pt_send.at[to], pt_recv.at[me],
                    p_send.at[rel * inner + k], p_recv.at[rel * inner + k], pa, px * 2 + pc, g))

    for rel in range(outer):
        for k in range(inner):
            pa, px, pc = peer(outer - rel, k)
            source = pa * inner + px * 2 + pc
            if rel == 0 and k == 0:
                part = nt_send[source]
            else:
                nc[rel, k].wait_recv()
                part = nt_recv[source]
            term = jnp.dot(part, keys(pa, px, pc), preferred_element_type=f32)
            if rel == 0 and k == 0:
                dacc[...] = term
            else:
                dacc[...] += term
    for i in range(per_row):
        dflat[pl.ds(i, height, stride=per_row), :] = dacc[:, i * LANE:(i + 1) * LANE]
    dflat[flat_rows:, :] = jnp.zeros((most, LANE), f32)
    wgrad_ref[...] = jnp.where(slot < count, dflat[pl.ds(offset, most), :], 0.0)

    for rel, k in pairs:
        pc_copies[rel, k].wait_recv()
    own[4].wait()
    feat[...] = jnp.zeros_like(feat)
    for o in range(owners):
        feat[windows[o]:windows[o] + height, :] += pt_recv[o].astype(f32)
    proj = jnp.zeros((tokens, LANE), f32)
    for i in range(chunks):
        cols = slice(i * LANE, (i + 1) * LANE)
        gained = gain_ref[:, cols] * (ngrad_ref[:, cols].astype(f32) + feat[cols, :].T)
        feat[cols, :] = gained
        proj = proj + gained * hidden_ref[:, cols].astype(f32)
    proj_sum = jnp.sum(proj, axis=1, keepdims=True)
    pj_send[...] = jnp.broadcast_to(proj_sum, (tokens, LANE)).T[0:8, :]
    pj_copy = start(remote(pj_send, pj_recv, e_send.at[1], e_recv.at[1], a, b, og))
    pj_copy.wait_recv()
    proj_all = proj_sum + jnp.broadcast_to(pj_recv[0:1, :], (tokens, LANE)).T[:, 0:1]
    scale = rstd * rstd * rstd * proj_all / model_width
    for i in range(chunks):
        cols = slice(i * LANE, (i + 1) * LANE)
        grad = feat[cols, :] * rstd - hidden_ref[:, cols].astype(f32) * scale
        hgrad_ref[:, cols] = grad.astype(bf16)
    for copy in sends:
        copy.wait_send()


def fast_plan(mesh, hidden, key, wb):
    outer, inner, halves = (mesh.shape[n] for n in ("gx", "gy", "gz"))
    tokens, rows, width, most = hidden.shape[0], hidden.shape[1], key.shape[1], wb.shape[2]
    if inner != 4 or halves != 2 or tokens != LANE or rows % LANE or width % LANE or most % 8:
        return None
    per_row = width // LANE
    windows, height = owner_windows(outer, inner, rows * per_row, most, per_row, rows)
    if rows % 16 or min(windows) < 0:
        return None
    held = outer * inner * (tokens * width * 2 + 4 * height * tokens * 2) + 6 * tokens * rows * 4
    if held > VMEM_BUDGET:
        return None
    return windows, height, per_row


def fast_shards(mesh, plan, hidden_in, norm_gain, normed_grad, key_grad, weight_blocks, block_count):
    windows, height, per_row = plan
    outer, inner = mesh.shape["gx"], mesh.shape["gy"]
    owners = outer * inner
    tokens, rows = hidden_in.shape
    width, most = key_grad.shape[1], weight_blocks.shape[2]
    model_width = rows * mesh.shape["gz"]
    flat_rows = height * per_row
    group = -(-rows * per_row // outer)
    pad = -(-max(
        i * group + min(j * most, group) - windows[i * inner + j] * per_row
        for i in range(outer) for j in range(inner)) // 8) * 8
    dims = (outer, inner, model_width, most, per_row, height, pad)
    f32, bf16 = jnp.float32, jnp.bfloat16
    vmem, dma = pltpu.VMEM, pltpu.SemaphoreType.DMA
    in_vmem = pl.BlockSpec(memory_space=pltpu.VMEM)
    in_hbm = pl.BlockSpec(memory_space=pltpu.HBM)
    hgrad, wgrad = pl.pallas_call(
        functools.partial(fast_kernel, dims, windows),
        out_shape=(jax.ShapeDtypeStruct((tokens, rows), bf16), jax.ShapeDtypeStruct((most, LANE), f32)),
        in_specs=[pl.BlockSpec(memory_space=pltpu.SMEM), in_hbm, in_vmem] + [in_hbm] * 3,
        out_specs=(in_vmem, in_vmem),
        scratch_shapes=[
            vmem((tokens, rows), bf16), vmem((tokens, rows), bf16), vmem((most, LANE), bf16),
            vmem((outer, 2, 2, 2, tokens // 2, width), bf16),
            vmem((owners, height, tokens), bf16), vmem((owners, height, tokens), bf16),
            vmem((owners, height, tokens), bf16), vmem((owners, height, tokens), bf16),
            vmem((rows, tokens), f32),
            vmem((pad + max(flat_rows, most), LANE), f32), vmem((flat_rows, LANE), f32),
            vmem((height, width), bf16), vmem((height, width), f32), vmem((flat_rows + most, LANE), f32),
            vmem((8, LANE), f32), vmem((8, LANE), f32), vmem((8, LANE), f32), vmem((8, LANE), f32),
            dma((5,)),
        ] + [dma((outer,))] * 8 + [dma((owners,))] * 4 + [dma((2,))] * 2,
        compiler_params=pltpu.CompilerParams(
            collective_id=0, has_side_effects=True),
    )(block_count, hidden_in, norm_gain.reshape(1, rows), normed_grad, key_grad,
      weight_blocks.reshape(most, LANE))
    return hgrad, wgrad.reshape(1, 1, most, LANE)


def block_layout(counts, blocks, owners, most):
    ends = jnp.cumsum(counts)
    starts = ends - counts
    block_ids = jnp.arange(blocks, dtype=jnp.int32)
    owner = jnp.searchsorted(ends, block_ids, side="right")
    gather_index = owner * most + block_ids - starts[owner]
    slot_owner = jnp.arange(owners * most, dtype=jnp.int32) // most
    slot_within = jnp.arange(owners * most, dtype=jnp.int32) % most
    valid = slot_within < counts[slot_owner]
    source = jnp.clip(starts[slot_owner] + slot_within, 0, blocks - 1)
    return (gather_index, source, valid)


def select_rows(index, keep, rows):
    columns = jnp.arange(rows.shape[0], dtype=jnp.int32)
    onehot = (index[:, None] == columns[None, :]) & keep[:, None]
    if rows.dtype == jnp.bfloat16:
        picked = jnp.dot(onehot.astype(jnp.bfloat16), rows, preferred_element_type=jnp.float32)
        return picked.astype(jnp.bfloat16)
    return jnp.dot(
        onehot.astype(jnp.float32),
        rows,
        precision=lax.Precision.HIGHEST,
        preferred_element_type=jnp.float32,
    )


def select_groups(index, keep, rows):

    def one_group(items):
        return select_rows(items[0], items[1], items[2])

    return lax.map(one_group, (index, keep, rows))


def shards(hidden_in, norm_gain, normed_grad, key_grad, weight_blocks, block_count):
    outer_size = lax.axis_size("gx")
    inner_size = lax.axis_size("gy")
    owners = outer_size * inner_size
    most = weight_blocks.shape[2]
    group_slots_count = inner_size * most
    group_rows = hidden_in.shape[1]
    width = key_grad.shape[1]
    blocks = group_rows * width // 128
    group_blocks = (blocks + outer_size - 1) // outer_size
    model_width = group_rows * lax.axis_size("gz")
    gather_index, source, valid = block_layout(block_count[0], blocks, owners, most)
    outer_index = lax.axis_index("gx")
    padded_index = jnp.pad(gather_index, (0, outer_size * group_blocks - blocks), mode="edge")
    group_offsets = jnp.arange(outer_size, dtype=jnp.int32)[:, None]
    local_index = jnp.clip(
        padded_index.reshape(outer_size, group_blocks) - group_offsets * group_slots_count,
        0,
        group_slots_count - 1,
    )
    local_source = jnp.clip(
        source.reshape(outer_size, group_slots_count) - group_offsets * group_blocks,
        0,
        group_blocks - 1,
    )
    local_valid = valid.reshape(outer_size, group_slots_count)
    all_rows = jnp.ones((outer_size, group_blocks), dtype=bool)
    local_blocks = weight_blocks.reshape(most, 128)
    gathered = lax.all_gather(local_blocks, ("gx", "gy"), axis=0, tiled=True)
    dense = select_groups(
        local_index, all_rows, gathered.reshape(outer_size, group_slots_count, 128)
    )
    weight = dense.reshape(outer_size * group_blocks, 128)[:blocks].reshape(group_rows, width)
    hfloat = hidden_in.astype(jnp.float32)
    squares = lax.psum(jnp.sum(hfloat * hfloat, axis=1), "gz")
    rstd = lax.rsqrt(squares / model_width + EPS)
    normed = (hfloat * rstd[:, None] * norm_gain).astype(jnp.bfloat16)
    dnorm = normed_grad.astype(jnp.float32) + lax.dot_general(
        key_grad, weight, (((1,), (1,)), ((), ())), preferred_element_type=jnp.float32
    )
    proj = lax.psum(jnp.sum(norm_gain * dnorm * hfloat, axis=1), "gz")
    grad = norm_gain * dnorm * rstd[:, None] - hfloat * (rstd**3 * proj / model_width)[:, None]
    hidden_grad = grad.astype(jnp.bfloat16)
    dweight = lax.dot_general(
        normed, key_grad, (((0,), (0,)), ((), ())), preferred_element_type=jnp.float32
    )
    flat = dweight.reshape(blocks, 128)
    flat_padded = jnp.pad(flat, ((0, outer_size * group_blocks - blocks), (0, 0)))
    group_sum = lax.psum_scatter(flat_padded, "gx", scatter_dimension=0, tiled=True)
    slot_source = lax.dynamic_index_in_dim(local_source, outer_index, 0, keepdims=False)
    slot_valid = lax.dynamic_index_in_dim(local_valid, outer_index, 0, keepdims=False)
    slotted = select_rows(slot_source, slot_valid, group_sum)
    owned = lax.psum_scatter(slotted, "gy", scatter_dimension=0, tiled=True)
    return (hidden_grad, owned.reshape(1, 1, most, 128))


def solution(mesh):
    placed = (
        P(("gx", "gy"), "gz"),
        P("gz"),
        P(("gx", "gy"), "gz"),
        P(("gx", "gy"), None),
        P(("gx", "gy"), "gz", None, None),
        P("gz", None),
    )

    def body(*args):
        plan = fast_plan(mesh, args[0], args[3], args[4])
        if plan is None:
            return shards(*args)
        return fast_shards(mesh, plan, *args)

    return jax.shard_map(
        body,
        mesh=mesh,
        in_specs=placed,
        out_specs=(P(("gx", "gy"), "gz"), P(("gx", "gy"), "gz", None, None)),
        check_vma=False,
    )
```
